32 devices in a mesh: grp: 2 (over y), row: 16 (over z, x, core).
Axes of the slice: x: 2, y: 2, z: 4, core: 2. Of those that a mesh axis runs over, the one named last changes fastest.
Arguments:
- cells: float32 [256, 128, 192], P(('grp', 'row')), parts along dimension 0, may hold values from -6 to 6
- n_train: int32 [2], P('grp'), parts along dimension 0, may hold values from 16 to 127
- present: int32 [256], P('grp'), parts along dimension 0, may hold values from 0 to 1, as said below
- norm_gain: float32 [3, 192], replicated, may hold values from 0.1 to 1.9
- feat_qkv: bfloat16 [3, 192, 192], replicated, may hold values from -6 to 6
- feat_out: bfloat16 [192, 192], replicated, may hold values from -0.4375 to 0.4375
- item_qkv: bfloat16 [3, 192, 192], replicated, may hold values from -6 to 6
- item_out: bfloat16 [192, 192], replicated, may hold values from -0.875 to 0.875
- mlp_in: bfloat16 [192, 768], replicated, may hold values from -0.4375 to 0.4375
- mlp_out: bfloat16 [768, 192], replicated, may hold values from -0.21875 to 0.21875
Outputs:
- result: float32 [256, 128, 192], P(('grp', 'row')), parts along dimension 0
The draws below stay inside these ranges and needn't reach their ends.
There are 2 independent parts, one for each index of `grp`. The reference program is written for one: setup_inputs(seed, part) draws one part's arguments, and reference() takes and returns one part's arrays. A program takes and returns all parts, laid end to end along the dimension named above; an argument that names none is the same for every part. Nothing has to cross between parts.
Inputs may be any that keep to these rules, and one draw needn't show every extreme that they name: At least one of the 128 features is present.
All inputs are finite; a program needn't handle non-finite values.
Results may differ from the reference program's by a relative error of at most 0.03.
The reference program's roundings to bfloat16 on the way count: a program that leaves them out, or rounds other values in their place, can miss the bound.
Values may be sent and summed in bfloat16 or wider, within the bound.
A program may use at most 64 MiB of HBM per device.

```python
import math
import jax
import jax.numpy as jnp
from jax import lax

E = 192
HEADS = 6
FF = 768
FEAT = 128
ROWS = 128


def drawn_triplet(key):
    base = jax.random.normal(key, (3, E, E), jnp.float32) / math.sqrt(E)
    stacked = jnp.stack([3.0 * base[0], 3.0 * base[1], base[2]])
    return jnp.clip(stacked, -6.0, 6.0).astype(jnp.bfloat16)


def draw_feat_qkv(key, part):
    return drawn_triplet(jax.random.fold_in(key, 11))


def draw_item_qkv(key, part):
    return drawn_triplet(jax.random.fold_in(key, 23))


def draw_present(key, part):
    levels = jax.random.randint(jax.random.fold_in(key, 5), (FEAT,), 0, 4)
    forced = jax.random.randint(jax.random.fold_in(key, 6), (), 0, FEAT)
    position = jnp.arange(FEAT, dtype=jnp.int32)
    return jnp.where((levels > 0) | (position == forced), 1, 0).astype(jnp.int32)


def block_levels(rng, dims, cuts, smallest, high):
    def one(dim, blocks):
        draws = jax.random.uniform(jax.random.fold_in(jax.random.fold_in(rng, 6), dim), (blocks,), jnp.float32, smallest / len(cuts), high / len(cuts))
        return jnp.repeat(jnp.exp(draws), dims[dim] // blocks).reshape((-1,) + (1,) * (len(dims) - dim - 1))

    loudness = one(*cuts[0])
    for cut in cuts[1:]:
        loudness = loudness * one(*cut)
    return loudness


def bell_draw(key, dims, width, bound, pieces=(), kind=jnp.bfloat16):
    values = jax.random.normal(key, dims, jnp.float32) * width
    if len(pieces) > 0:
        values = block_levels(key, dims, pieces, -0.22, 0.18) * values
    return jnp.clip(values, min=-bound, max=bound).astype(kind)


def setup_inputs(seed: int = 0, part: int = 0) -> dict:
    splits = jax.random.split(jax.random.key(seed), 11)
    own_keys = jax.random.split(jax.random.fold_in(splits[10], part), 11)
    return {
        "cells": bell_draw(own_keys[0], (ROWS, FEAT, E), 1.0, 6.0, ((0, 16),), jnp.float32),
        "n_train": jax.random.randint(own_keys[1], (1,), ROWS // 8, ROWS).astype(jnp.int32),
        "present": draw_present(jax.random.fold_in(jax.random.fold_in(splits[10], part), 71), part),
        "norm_gain": jnp.clip(1.0 + 0.18 * jax.random.normal(splits[3], (3, E), jnp.float32), 0.1, 1.9),
        "feat_qkv": draw_feat_qkv(jax.random.fold_in(splits[10], 71), part),
        "feat_out": bell_draw(splits[5], (E, E), E ** -0.5, 0.4375),
        "item_qkv": draw_item_qkv(jax.random.fold_in(splits[10], 71), part),
        "item_out": bell_draw(splits[7], (E, E), (E // 4) ** -0.5, 0.875),
        "mlp_in": bell_draw(splits[8], (E, FF), E ** -0.5, 0.4375),
        "mlp_out": bell_draw(splits[9], (FF, E), FF ** -0.5, 0.21875),
    }


norm_floor = 0.25
masked_score = -1e+30

def widen(array):
    return array.astype(jnp.float32)

def layer_norm(stream, gain):
    average = lax.optimization_barrier(jnp.mean(stream, axis=-1, keepdims=True))
    centred = stream - average
    spread = lax.optimization_barrier(jnp.mean(centred * centred, axis=-1, keepdims=True))
    return centred * lax.rsqrt(spread + norm_floor) * gain

def softmax_rows(scores):
    largest = lax.optimization_barrier(jnp.max(scores, axis=-1, keepdims=True))
    exponent = jnp.exp(scores - largest)
    return exponent / lax.optimization_barrier(jnp.sum(exponent, axis=-1, keepdims=True))

def reference(cells, n_train, present, norm_gain, feat_qkv, feat_out, item_qkv, item_out, mlp_in, mlp_out):
    head_size = E // HEADS
    scale = 1.0 / math.sqrt(head_size)
    row_group = math.gcd(ROWS, 128)
    query_rows = min(512, ROWS)
    highest = lax.Precision.HIGHEST

    def feature_group(stream):
        normed = layer_norm(stream, norm_gain[0]).astype(jnp.bfloat16)
        triplet = jnp.einsum('rfe,ced->crfd', widen(normed), widen(feat_qkv))
        triplet = triplet.reshape(3, row_group, FEAT, HEADS, head_size)
        values = widen(triplet[2].astype(jnp.bfloat16))
        scores = jnp.einsum('rfhd,rghd->rhfg', triplet[0], triplet[1], precision=highest) * scale
        scores = jnp.where(present[None, None, None, :] > 0, scores, masked_score)
        weights = softmax_rows(scores).astype(jnp.bfloat16)
        context = jnp.einsum('rhfg,rghd->rfhd', widen(weights), values).astype(jnp.bfloat16)
        context = context.reshape(row_group, FEAT, E)
        return stream + jnp.dot(context, feat_out, preferred_element_type=jnp.float32)
    cells_mid = lax.map(feature_group, cells.reshape(ROWS // row_group, row_group, FEAT, E)).reshape(ROWS, FEAT, E)
    key_live = jnp.arange(ROWS, dtype=jnp.int32) < n_train[0]

    def item_feature(stream):
        normed = layer_norm(stream, norm_gain[1]).astype(jnp.bfloat16)
        triplet = jnp.einsum('re,ced->crd', widen(normed), widen(item_qkv))
        keys = triplet[1].reshape(ROWS, HEADS, head_size)
        values = widen(triplet[2].astype(jnp.bfloat16)).reshape(ROWS, HEADS, head_size)
        queries = triplet[0].reshape(ROWS // query_rows, query_rows, HEADS, head_size)

        def query_group(chosen):
            scores = jnp.einsum('qhd,shd->hqs', chosen, keys, precision=highest) * scale
            scores = jnp.where(key_live[None, None, :], scores, masked_score)
            weights = softmax_rows(scores).astype(jnp.bfloat16)
            return jnp.einsum('hqs,shd->qhd', widen(weights), values).astype(jnp.bfloat16)
        context = lax.map(query_group, queries).reshape(ROWS, E)
        late = stream + jnp.dot(context, item_out, preferred_element_type=jnp.float32)
        normed_late = layer_norm(late, norm_gain[2]).astype(jnp.bfloat16)
        hidden = jax.nn.gelu(jnp.dot(normed_late, mlp_in, preferred_element_type=jnp.float32), approximate=False).astype(jnp.bfloat16)
        return late + jnp.dot(hidden, mlp_out, preferred_element_type=jnp.float32)
    updated = lax.map(item_feature, jnp.transpose(cells_mid, (1, 0, 2)))
    return jnp.transpose(updated, (1, 0, 2))
```

```python
import functools
import math

import jax
import jax.numpy as jnp
from jax import lax
from jax.experimental import pallas as pl
from jax.experimental.pallas import tpu as pltpu
from jax.sharding import PartitionSpec as P

HEADS = 6
LANES = 128
SUBLANES = 8


norm_floor = 0.25
masked_score = -1e30


def layer_norm(stream, gain):
    average = jnp.mean(stream, axis=-1, keepdims=True)
    centred = stream - average
    spread = jnp.mean(centred * centred, axis=-1, keepdims=True)
    return centred * lax.rsqrt(spread + norm_floor) * gain


def softmax_rows(scores):
    largest = jnp.max(scores, axis=-1, keepdims=True)
    exponent = jnp.exp(scores - largest)
    return exponent / jnp.sum(exponent, axis=-1, keepdims=True)


def plain_body(
    cells, n_train, present, norm_gain, feat_qkv, feat_out, item_qkv, item_out, mlp_in, mlp_out
):
    row_dev, feature_count, model_width = cells.shape
    devices_row = lax.axis_size("row")
    total_rows = row_dev * devices_row
    feat_dev = feature_count // devices_row
    head_size = model_width // HEADS
    scale = 1.0 / math.sqrt(head_size)
    query_rows = min(512, total_rows)
    highest = lax.Precision.HIGHEST
    normed = layer_norm(cells, norm_gain[0]).astype(jnp.bfloat16)
    triplet = jnp.einsum("rfe,ced->crfd", normed, feat_qkv, preferred_element_type=jnp.float32)
    triplet = triplet.reshape(3, row_dev, feature_count, HEADS, head_size)
    feat_values = triplet[2].astype(jnp.bfloat16)
    scores = jnp.einsum("rfhd,rghd->rhfg", triplet[0], triplet[1], precision=highest) * scale
    scores = jnp.where(present[None, None, None, :] > 0, scores, masked_score)
    weights = softmax_rows(scores).astype(jnp.bfloat16)
    context = jnp.einsum(
        "rhfg,rghd->rfhd", weights, feat_values, preferred_element_type=jnp.float32
    ).astype(jnp.bfloat16)
    context = context.reshape(row_dev, feature_count, model_width)
    cells_mid = cells + jnp.dot(context, feat_out, preferred_element_type=jnp.float32)
    key_live = lax.iota(jnp.int32, total_rows) < n_train[0]
    arrived = lax.all_to_all(
        cells_mid.reshape(row_dev, devices_row, feat_dev, model_width).astype(jnp.bfloat16),
        "row",
        split_axis=1,
        concat_axis=0,
        tiled=True,
    ).astype(jnp.float32)
    members = arrived.shape[2]
    stream = arrived.reshape(total_rows, members, model_width)
    normed_rows = layer_norm(stream, norm_gain[1]).astype(jnp.bfloat16)
    triples = jnp.einsum("rke,ced->kcrd", normed_rows, item_qkv, preferred_element_type=jnp.float32)

    def one_feature(triple):
        keys = triple[1].reshape(total_rows, HEADS, head_size)
        values = triple[2].astype(jnp.bfloat16).reshape(total_rows, HEADS, head_size)
        queries = triple[0].reshape(total_rows // query_rows, query_rows, HEADS, head_size)

        def query_group(chosen):
            group_scores = jnp.einsum("qhd,shd->hqs", chosen, keys, precision=highest) * scale
            group_scores = jnp.where(key_live[None, None, :], group_scores, masked_score)
            group_weights = softmax_rows(group_scores).astype(jnp.bfloat16)
            return jnp.einsum(
                "hqs,shd->qhd", group_weights, values, preferred_element_type=jnp.float32
            ).astype(jnp.bfloat16)

        return lax.map(query_group, queries).reshape(total_rows, model_width)

    gathered = lax.map(one_feature, triples)
    late = stream + jnp.dot(
        jnp.transpose(gathered, (1, 0, 2)), item_out, preferred_element_type=jnp.float32
    )
    normed_late = layer_norm(late, norm_gain[2]).astype(jnp.bfloat16)
    hidden = jax.nn.gelu(
        jnp.dot(normed_late, mlp_in, preferred_element_type=jnp.float32), approximate=False
    ).astype(jnp.bfloat16)
    updated = late + jnp.dot(hidden, mlp_out, preferred_element_type=jnp.float32)
    returned = lax.all_to_all(
        updated.reshape(total_rows, 1, members, model_width).astype(jnp.bfloat16),
        "row",
        split_axis=0,
        concat_axis=1,
        tiled=True,
    ).astype(jnp.float32)
    return returned.reshape(row_dev, feature_count, model_width)


def matmul(left, right, dims=(1, 0)):
    return lax.dot_general(
        left, right, (((dims[0],), (dims[1],)), ((), ())), preferred_element_type=jnp.float32
    )


def pick_rows(width, total):
    down = lax.broadcasted_iota(jnp.int32, (width, total), 0)
    across = lax.broadcasted_iota(jnp.int32, (width, total), 1)
    source = jnp.where(across < width, across, across - (total - width))
    return jnp.where(down == source, 1.0, 0.0).astype(jnp.bfloat16)


def turn(weight, total):
    return matmul(weight, pick_rows(weight.shape[0], total), (0, 0)).astype(jnp.bfloat16)


def prepare_weights(qkv_ref, turned_ref, spread_ref):
    width = qkv_ref.shape[1]
    total = turned_ref.shape[1]
    head = width // HEADS
    turned_ref[:width, :] = turn(qkv_ref[0], total)
    turned_ref[width:, :] = turn(qkv_ref[2], total)
    down = lax.broadcasted_iota(jnp.int32, (width, 4 * width), 0)
    across = lax.broadcasted_iota(jnp.int32, (width, 4 * width), 1)
    source = (across // (4 * head)) * head + across % head
    pick = jnp.where(down == source, 1.0, 0.0).astype(jnp.bfloat16)
    spread = matmul(qkv_ref[1], pick).astype(jnp.bfloat16)
    spread_ref[:width, :] = spread
    if total > width:
        spread_ref[width:, :] = spread[2 * width - total :]


def attention(turned, keys, bias_ref):
    width = turned.shape[0] // 2
    tokens = turned.shape[1]
    size = bias_ref.shape[0]
    head = width // HEADS
    wide = 4 * head
    queries = turned[:width] * (math.log2(math.e) / math.sqrt(head))
    query_high = queries.astype(jnp.bfloat16)
    query_low = (queries - query_high.astype(jnp.float32)).astype(jnp.bfloat16)
    values = turned[width:].astype(jnp.bfloat16)
    lane = lax.broadcasted_iota(jnp.int32, (1, 4 * width), 1)
    rounded = keys.astype(jnp.bfloat16).astype(jnp.float32)
    keys = jnp.where(lane % wide < 2 * head, keys, keys - rounded).astype(jnp.bfloat16)
    blocks = []
    for block in range(tokens // size):
        here = slice(block * size, (block + 1) * size)
        contexts = []
        for h in range(HEADS):
            rows = slice(h * head, (h + 1) * head)
            high, low = query_high[rows, here], query_low[rows, here]
            query = jnp.concatenate([high, low, high, low], axis=0)
            scores = matmul(keys[here, h * wide : (h + 1) * wide], query) + bias_ref[...]
            exponent = jnp.exp2(scores - jnp.max(scores, axis=0, keepdims=True))
            share = 1.0 / jnp.sum(exponent, axis=0, keepdims=True)
            weights = (exponent * share).astype(jnp.bfloat16)
            contexts.append(matmul(values[rows, here], weights))
        blocks.append(jnp.concatenate(contexts, axis=0))
    return blocks


def norm_down(stream, gain):
    average = jnp.mean(stream, axis=0, keepdims=True)
    centred = stream - average
    spread = jnp.mean(centred * centred, axis=0, keepdims=True)
    return centred * lax.rsqrt(spread + norm_floor) * gain


def kernel(
    devices,
    n_train_ref, cells_ref, present_hbm, gain_hbm, feat_qkv_hbm, feat_out_hbm, item_qkv_hbm,
    item_out_hbm, mlp_in_hbm, mlp_out_hbm,
    out_ref,
    present_ref, gain_ref, feat_qkv_ref, feat_out_ref, item_qkv_ref, item_out_ref, mlp_in_ref,
    mlp_out_ref, turned_f, spread_f, turned_i, spread_i, out_f, out_i, into, gains, bias_f, bias_i,
    mid, sort_a, sort_b, sort_i, loose_a, loose_b, send, recv, back, home, in_sem, send_sem, recv_sem,
    back_sem, home_sem,
):
    me = lax.axis_index("row")
    rows, width, feats = cells_ref.shape
    steps = rows // 2
    half = rows // 2
    group = feats // 2
    share = group // devices
    total_rows = rows * devices
    rest = width - LANES
    order = range(1, devices)
    others = pl.ds(0, devices - 1)

    barrier = pltpu.get_barrier_semaphore()
    for shift in order:
        pl.semaphore_signal(
            barrier, inc=1, device_id={"row": lax.rem(me + shift, devices)},
            device_id_type=pl.DeviceIdType.MESH,
        )

    moves = [
        (gain_hbm, gain_ref), (present_hbm, present_ref), (feat_qkv_hbm, feat_qkv_ref),
        (cells_ref.at[pl.ds(0, half)], mid.at[pl.ds(0, half)]), (feat_out_hbm, feat_out_ref),
        (cells_ref.at[pl.ds(half, half)], mid.at[pl.ds(half, half)]),
        (item_qkv_hbm, item_qkv_ref), (item_out_hbm, item_out_ref), (mlp_in_hbm, mlp_in_ref),
        (mlp_out_hbm, mlp_out_ref),
    ]
    loads = [
        pltpu.make_async_copy(source, target, in_sem.at[number])
        for number, (source, target) in enumerate(moves)
    ]
    for load in loads:
        load.start()

    def outgoing(part, side, shift, slots):
        to = lax.rem(me + shift, devices)
        return pltpu.make_async_remote_copy(
            src_ref=send.at[part, side, to if slots is None else slots],
            dst_ref=recv.at[part, side, me if slots is None else slots],
            send_sem=send_sem.at[part, side], recv_sem=recv_sem.at[part, side],
            device_id={"row": to}, device_id_type=pl.DeviceIdType.MESH,
        )

    def returning(side, pair, shift, slots):
        to = lax.rem(me + shift, devices)
        return pltpu.make_async_remote_copy(
            src_ref=back.at[side, pair, to if slots is None else slots],
            dst_ref=home.at[side, pair, me if slots is None else slots],
            send_sem=back_sem.at[side, pair], recv_sem=home_sem.at[side, pair],
            device_id={"row": to}, device_id_type=pl.DeviceIdType.MESH,
        )

    def turned_parts(one, two):
        last = jnp.concatenate([one[LANES:], two[LANES:]], axis=0)
        return [part.T for part in (one[:LANES], two[:LANES], last)]

    def keep(tile, one):
        left = lax.broadcasted_iota(jnp.int32, tile.shape, 1) < rest
        return jnp.where(left if one == 0 else jnp.logical_not(left), tile, 0.0)

    for load in loads[:3]:
        load.wait()
    for number in range(3):
        gains[number] = jnp.broadcast_to(gain_ref[number : number + 1, :], (feats, width)).T
    live = jnp.where(present_ref[...] > 0, 0.0, masked_score)
    bias_f[...] = jnp.broadcast_to(live, (feats, feats)).T
    prepare_weights(feat_qkv_ref, turned_f, spread_f)

    def gain_of(number):
        return jnp.concatenate([gains[number], gains[number]], axis=1)

    def feature_rows(step):
        cells = jnp.concatenate([mid[2 * step], mid[2 * step + 1]], axis=1)
        normed = norm_down(cells, gain_of(0)).astype(jnp.bfloat16)
        turned = matmul(turned_f[...], normed)
        keys = matmul(normed, spread_f[...], (0, 0))
        contexts = attention(turned, keys, bias_f)
        context = jnp.concatenate(contexts, axis=1).astype(jnp.bfloat16)
        updated = cells + matmul(out_f[...], context)
        mid[2 * step] = updated[:, :feats]
        mid[2 * step + 1] = updated[:, feats:]
        normed = norm_down(updated, gain_of(1))
        parts = turned_parts(normed[:, :feats], normed[:, feats:])
        part, inner = 2 * step // half, 2 * step % half
        for side in range(2):
            here = slice(side * group, (side + 1) * group)
            for one in range(2):
                sort_a[part, side, pl.ds(inner + one, group, stride=half), :] = parts[one][here]
            sort_b[part, side, pl.ds(inner // 2, group, stride=half // 2), :] = parts[2][here]

    def dispatch(part, side):
        for shift in order:
            outgoing(part, side, shift, None).start()
        recv[part, side, me] = send[part, side, me]

    for part in range(2):
        if part == 0:
            loads[3].wait()
            loads[4].wait()
            out_f[...] = turn(feat_out_ref[...], width)
        else:
            loads[5].wait()
        for step in range(part * steps // 2, (part + 1) * steps // 2):
            feature_rows(step)
        for side in range(2):
            first = sort_a[part, side].reshape(devices, share * half, LANES)
            last = sort_b[part, side].reshape(devices, share * half // 2, LANES)
            send[part, side, :, : share * half] = first.astype(jnp.bfloat16)
            send[part, side, :, share * half :] = last.astype(jnp.bfloat16)
        if part == 0:
            pl.semaphore_wait(barrier, devices - 1)
            dispatch(0, 0)
    dispatch(1, 0)
    dispatch(0, 1)
    dispatch(1, 1)

    for load in loads[6:]:
        load.wait()
    prepare_weights(item_qkv_ref, turned_i, spread_i)
    out_i[...] = turn(item_out_ref[...], out_i.shape[1])
    into[...] = turn(mlp_in_ref[...], width)
    token = lax.broadcasted_iota(jnp.int32, (total_rows, total_rows), 0)
    number = token % devices * rows + token // devices
    bias_i[...] = jnp.where(number < n_train_ref[0], 0.0, masked_score)

    def item_side(side, carry):
        for part in range(2):
            outgoing(part, side, 1, others).wait_recv()
            tiles = recv[part, side].astype(jnp.float32)
            for device in range(devices):
                start = (device * 2 + part) * share * half
                loose_a[start : start + share * half, :] = tiles[device, : share * half]
                for one in range(2):
                    put = pl.ds(start + one, share * half // 2, stride=2)
                    loose_b[put, :] = keep(tiles[device, share * half :], one)

        def collect(feature):
            pieces = []
            for row in range(rows):
                start = (row // half) * share * half + feature * half + row % half
                take = pl.ds(start, devices, stride=2 * share * half)
                pieces.append(jnp.concatenate([loose_a[take, :], loose_b[take, :]], axis=1))
            return jnp.concatenate(pieces, axis=0)

        for pair in range(2):
            normed = jnp.concatenate([collect(2 * pair), collect(2 * pair + 1)], axis=0)
            normed = normed.astype(jnp.bfloat16)
            turned = matmul(turned_i[...], normed, (1, 1))
            keys = matmul(normed, spread_i[...])
            parts = turned_parts(*attention(turned, keys, bias_i))
            for number, part in enumerate(parts):
                sort_i[pair, number] = part
            for device in range(devices):
                take = pl.ds(device, rows, stride=devices)
                tile = jnp.concatenate([sort_i[pair, n, take, :] for n in range(3)], axis=0)
                back[side, pair, device] = tile.astype(jnp.bfloat16)
            for shift in order:
                returning(side, pair, shift, None).start()
            home[side, pair, me] = back[side, pair, me]
        return carry

    lax.fori_loop(0, 2, item_side, 0)

    def finish_side(side):
        for pair in range(2):
            returning(side, pair, 1, others).wait_recv()
            tiles = home[side, pair].astype(jnp.float32)
            for device in range(devices):
                for one in range(2):
                    start = (device * share + 2 * pair + one) * rows
                    loose_a[start : start + rows, :] = tiles[device, one * rows : (one + 1) * rows]
                    loose_b[start : start + rows, :] = keep(tiles[device, 2 * rows :], one)
        here = slice(side * group, (side + 1) * group)
        for first in range(0, rows, 4):
            chosen = range(first, first + 4)
            context = []
            for row in chosen:
                take = pl.ds(row, group, stride=rows)
                context.append(jnp.concatenate([loose_a[take, :], loose_b[take, :]], axis=1))
            context = jnp.concatenate(context, axis=0).astype(jnp.bfloat16)
            stream = jnp.concatenate([mid[row, :, here] for row in chosen], axis=1)
            late = stream + matmul(out_i[...], context, (1, 1))
            normed = norm_down(late, gain_of(2)).astype(jnp.bfloat16)
            inner = matmul(into[...], normed)
            hidden = (0.5 * inner * (1.0 + lax.erf(inner * math.sqrt(0.5)))).astype(jnp.bfloat16)
            done = late + matmul(mlp_out_ref[...], hidden)
            for number, row in enumerate(chosen):
                out_ref[row, :, here] = done[:, number * group : (number + 1) * group]

    for side in range(2):
        finish_side(side)
    for part in range(2):
        for side in range(2):
            outgoing(part, side, 1, others).wait_send()
            returning(part, side, 1, others).wait_send()


def body(
    cells, n_train, present, norm_gain, feat_qkv, feat_out, item_qkv, item_out, mlp_in, mlp_out
):
    devices = lax.axis_size("row")
    rows, feats, width = cells.shape
    feat_dev = feats // devices
    fits = rows == SUBLANES and feat_dev == SUBLANES and 2 * width == 3 * LANES
    fits = fits and rows * devices == LANES and feats == LANES and width % (HEADS * 16) == 0
    if not fits:
        return plain_body(
            cells, n_train, present, norm_gain, feat_qkv, feat_out, item_qkv, item_out, mlp_in,
            mlp_out,
        )
    total_rows = rows * devices
    hidden = mlp_in.shape[1]
    total = 2 * LANES
    vmem = pl.BlockSpec(memory_space=pltpu.VMEM)
    hbm = pl.BlockSpec(memory_space=pltpu.HBM)
    bf16, f32 = jnp.bfloat16, jnp.float32
    slots = pltpu.VMEM((2, 2, devices, 3 * rows, LANES), bf16)
    sems = pltpu.SemaphoreType.DMA((2, 2))
    loose = pltpu.VMEM((rows * feats // 2, LANES), f32)
    arrays = (
        jnp.swapaxes(cells, 1, 2), present.reshape(1, feats), norm_gain, feat_qkv, feat_out,
        item_qkv, item_out, mlp_in, mlp_out.T,
    )
    arrays = [pltpu.with_memory_space_constraint(array, pltpu.HBM) for array in arrays]
    out = pl.pallas_call(
        functools.partial(kernel, devices),
        out_shape=jax.ShapeDtypeStruct((rows, width, feats), f32),
        in_specs=[pl.BlockSpec(memory_space=pltpu.SMEM)] + [hbm] * 9,
        out_specs=vmem,
        scratch_shapes=[
            pltpu.VMEM((1, feats), jnp.int32),
            pltpu.VMEM((3, width), f32),
            pltpu.VMEM((3, width, width), bf16),
            pltpu.VMEM((width, width), bf16),
            pltpu.VMEM((3, width, width), bf16),
            pltpu.VMEM((width, width), bf16),
            pltpu.VMEM((width, hidden), bf16),
            pltpu.VMEM((width, hidden), bf16),
            pltpu.VMEM((2 * width, width), bf16),
            pltpu.VMEM((width, 4 * width), bf16),
            pltpu.VMEM((2 * width, total), bf16),
            pltpu.VMEM((total, 4 * width), bf16),
            pltpu.VMEM((width, width), bf16),
            pltpu.VMEM((width, total), bf16),
            pltpu.VMEM((hidden, width), bf16),
            pltpu.VMEM((3, width, feats), f32),
            pltpu.VMEM((feats, feats), f32),
            pltpu.VMEM((total_rows, total_rows), f32),
            pltpu.VMEM((rows, width, feats), f32),
            pltpu.VMEM((2, 2, rows * feats // 4, LANES), f32),
            pltpu.VMEM((2, 2, rows * feats // 8, LANES), f32),
            pltpu.VMEM((2, 3, total_rows, LANES), f32),
            loose, loose, slots, slots, slots, slots,
            pltpu.SemaphoreType.DMA((10,)),
            sems, sems, sems, sems,
        ],
        compiler_params=pltpu.CompilerParams(
            collective_id=0, has_side_effects=True, vmem_limit_bytes=48 * 1024 * 1024
        ),
    )(n_train, *arrays)
    return jnp.swapaxes(out, 1, 2)


def solution(mesh):
    return jax.shard_map(
        body,
        mesh=mesh,
        in_specs=(
            P(("grp", "row"), None, None),
            P("grp"),
            P("grp"),
            P(),
            P(),
            P(),
            P(),
            P(),
            P(),
            P(),
        ),
        out_specs=P(("grp", "row"), None, None),
        check_vma=False,
    )
```

```python
import functools
import math

import jax
import jax.numpy as jnp
from jax import lax
from jax.experimental import pallas as pl
from jax.experimental.pallas import tpu as pltpu
from jax.sharding import PartitionSpec as P

HEADS = 6
LANES = 128
SUBLANES = 8


norm_floor = 0.25
masked_score = -1e30


def layer_norm(stream, gain):
    average = jnp.mean(stream, axis=-1, keepdims=True)
    centred = stream - average
    spread = jnp.mean(centred * centred, axis=-1, keepdims=True)
    return centred * lax.rsqrt(spread + norm_floor) * gain


def softmax_rows(scores):
    largest = jnp.max(scores, axis=-1, keepdims=True)
    exponent = jnp.exp(scores - largest)
    return exponent / jnp.sum(exponent, axis=-1, keepdims=True)


def plain_body(
    cells, n_train, present, norm_gain, feat_qkv, feat_out, item_qkv, item_out, mlp_in, mlp_out
):
    row_dev, feature_count, model_width = cells.shape
    devices_row = lax.axis_size("row")
    total_rows = row_dev * devices_row
    feat_dev = feature_count // devices_row
    head_size = model_width // HEADS
    scale = 1.0 / math.sqrt(head_size)
    query_rows = min(512, total_rows)
    highest = lax.Precision.HIGHEST
    normed = layer_norm(cells, norm_gain[0]).astype(jnp.bfloat16)
    triplet = jnp.einsum("rfe,ced->crfd", normed, feat_qkv, preferred_element_type=jnp.float32)
    triplet = triplet.reshape(3, row_dev, feature_count, HEADS, head_size)
    feat_values = triplet[2].astype(jnp.bfloat16)
    scores = jnp.einsum("rfhd,rghd->rhfg", triplet[0], triplet[1], precision=highest) * scale
    scores = jnp.where(present[None, None, None, :] > 0, scores, masked_score)
    weights = softmax_rows(scores).astype(jnp.bfloat16)
    context = jnp.einsum(
        "rhfg,rghd->rfhd", weights, feat_values, preferred_element_type=jnp.float32
    ).astype(jnp.bfloat16)
    context = context.reshape(row_dev, feature_count, model_width)
    cells_mid = cells + jnp.dot(context, feat_out, preferred_element_type=jnp.float32)
    key_live = lax.iota(jnp.int32, total_rows) < n_train[0]
    arrived = lax.all_to_all(
        cells_mid.reshape(row_dev, devices_row, feat_dev, model_width).astype(jnp.bfloat16),
        "row",
        split_axis=1,
        concat_axis=0,
        tiled=True,
    ).astype(jnp.float32)
    members = arrived.shape[2]
    stream = arrived.reshape(total_rows, members, model_width)
    normed_rows = layer_norm(stream, norm_gain[1]).astype(jnp.bfloat16)
    triples = jnp.einsum("rke,ced->kcrd", normed_rows, item_qkv, preferred_element_type=jnp.float32)

    def one_feature(triple):
        keys = triple[1].reshape(total_rows, HEADS, head_size)
        values = triple[2].astype(jnp.bfloat16).reshape(total_rows, HEADS, head_size)
        queries = triple[0].reshape(total_rows // query_rows, query_rows, HEADS, head_size)

        def query_group(chosen):
            group_scores = jnp.einsum("qhd,shd->hqs", chosen, keys, precision=highest) * scale
            group_scores = jnp.where(key_live[None, None, :], group_scores, masked_score)
            group_weights = softmax_rows(group_scores).astype(jnp.bfloat16)
            return jnp.einsum(
                "hqs,shd->qhd", group_weights, values, preferred_element_type=jnp.float32
            ).astype(jnp.bfloat16)

        return lax.map(query_group, queries).reshape(total_rows, model_width)

    gathered = lax.map(one_feature, triples)
    late = stream + jnp.dot(
        jnp.transpose(gathered, (1, 0, 2)), item_out, preferred_element_type=jnp.float32
    )
    normed_late = layer_norm(late, norm_gain[2]).astype(jnp.bfloat16)
    hidden = jax.nn.gelu(
        jnp.dot(normed_late, mlp_in, preferred_element_type=jnp.float32), approximate=False
    ).astype(jnp.bfloat16)
    updated = late + jnp.dot(hidden, mlp_out, preferred_element_type=jnp.float32)
    returned = lax.all_to_all(
        updated.reshape(total_rows, 1, members, model_width).astype(jnp.bfloat16),
        "row",
        split_axis=0,
        concat_axis=1,
        tiled=True,
    ).astype(jnp.float32)
    return returned.reshape(row_dev, feature_count, model_width)


def matmul(left, right, dims=(1, 0)):
    return lax.dot_general(
        left, right, (((dims[0],), (dims[1],)), ((), ())), preferred_element_type=jnp.float32
    )


def pick_rows(width, total):
    down = lax.broadcasted_iota(jnp.int32, (width, total), 0)
    across = lax.broadcasted_iota(jnp.int32, (width, total), 1)
    source = jnp.where(across < width, across, across - (total - width))
    return jnp.where(down == source, 1.0, 0.0).astype(jnp.bfloat16)


def turn(weight, total):
    return matmul(weight, pick_rows(weight.shape[0], total), (0, 0)).astype(jnp.bfloat16)


def prepare_weights(qkv_ref, turned_ref, spread_ref):
    width = qkv_ref.shape[1]
    total = turned_ref.shape[1]
    head = width // HEADS
    turned_ref[:width, :] = turn(qkv_ref[0], total)
    turned_ref[width:, :] = turn(qkv_ref[2], total)
    down = lax.broadcasted_iota(jnp.int32, (width, 2 * width), 0)
    across = lax.broadcasted_iota(jnp.int32, (width, 2 * width), 1)
    source = (across // (2 * head)) * head + across % head
    pick = jnp.where(down == source, 1.0, 0.0).astype(jnp.bfloat16)
    spread = matmul(qkv_ref[1], pick).astype(jnp.bfloat16)
    spread_ref[:width, :] = spread
    if total > width:
        spread_ref[width:, :] = spread[2 * width - total :]


def split(wide):
    high = wide.astype(jnp.bfloat16)
    return high, (wide - high.astype(jnp.float32)).astype(jnp.bfloat16)


def attention(turned, keys, bias_ref):
    width = turned.shape[0] // 2
    tokens = turned.shape[1]
    size = bias_ref.shape[0]
    head = width // HEADS
    query_high, query_low = split(turned[:width] * (math.log2(math.e) / math.sqrt(head)))
    key_high, key_low = split(keys)
    values = turned[width:].astype(jnp.bfloat16)
    zero = jnp.zeros((2 * head, size), jnp.bfloat16)
    blocks = []
    for block in range(tokens // size):
        here = slice(block * size, (block + 1) * size)
        contexts = []
        for pair in range(HEADS // 2):
            query = []
            for h in (2 * pair, 2 * pair + 1):
                rows = slice(h * head, (h + 1) * head)
                one = jnp.concatenate([query_high[rows, here], query_low[rows, here]], axis=0)
                both = [one, zero] if h % 2 == 0 else [zero, one]
                query.append(jnp.concatenate(both, axis=1))
            query = jnp.concatenate(query + query, axis=0)
            lanes = slice(pair * 4 * head, (pair + 1) * 4 * head)
            key = jnp.concatenate([key_high[here, lanes], key_low[here, lanes]], axis=1)
            both = matmul(key, query)
            for one in range(2):
                rows = slice((2 * pair + one) * head, (2 * pair + one + 1) * head)
                scores = both[:, one * size : (one + 1) * size] + bias_ref[...]
                exponent = jnp.exp2(scores - jnp.max(scores, axis=0, keepdims=True))
                share = 1.0 / jnp.sum(exponent, axis=0, keepdims=True)
                weights = (exponent * share).astype(jnp.bfloat16)
                contexts.append(matmul(values[rows, here], weights))
        blocks.append(jnp.concatenate(contexts, axis=0))
    return blocks


def norm_down(stream, gain):
    average = jnp.mean(stream, axis=0, keepdims=True)
    centred = stream - average
    spread = jnp.mean(centred * centred, axis=0, keepdims=True)
    return centred * lax.rsqrt(spread + norm_floor) * gain


def kernel(
    devices,
    n_train_ref, cells_ref, present_hbm, gain_hbm, feat_qkv_hbm, feat_out_hbm, item_qkv_hbm,
    item_out_hbm, mlp_in_hbm, mlp_out_hbm,
    out_ref,
    present_ref, gain_ref, feat_qkv_ref, feat_out_ref, item_qkv_ref, item_out_ref, mlp_in_ref,
    mlp_out_ref, turned_f, spread_f, turned_i, spread_i, out_f, out_i, into, gains, bias_f, bias_i,
    mid, paired, sort_a, sort_b, sort_i, loose_a, loose_b, send, recv, back, home, in_sem, send_sem, recv_sem,
    back_sem, home_sem,
):
    me = lax.axis_index("row")
    rows, width, feats = cells_ref.shape
    steps = rows // 2
    half = rows // 2
    group = feats // 2
    share = group // devices
    total_rows = rows * devices
    rest = width - LANES
    order = range(1, devices)
    others = pl.ds(0, devices - 1)

    moves = [
        (gain_hbm, gain_ref), (present_hbm, present_ref), (feat_qkv_hbm, feat_qkv_ref),
        (cells_ref.at[pl.ds(0, half)], mid.at[pl.ds(0, half)]), (feat_out_hbm, feat_out_ref),
        (cells_ref.at[pl.ds(half, half)], mid.at[pl.ds(half, half)]),
        (item_qkv_hbm, item_qkv_ref), (item_out_hbm, item_out_ref), (mlp_in_hbm, mlp_in_ref),
        (mlp_out_hbm, mlp_out_ref),
    ]
    loads = [
        pltpu.make_async_copy(source, target, in_sem.at[number])
        for number, (source, target) in enumerate(moves)
    ]
    for load in loads[:5]:
        load.start()

    barrier = pltpu.get_barrier_semaphore()
    for shift in order:
        pl.semaphore_signal(
            barrier, inc=1, device_id={"row": lax.rem(me + shift, devices)},
            device_id_type=pl.DeviceIdType.MESH,
        )
    for load in loads[5:]:
        load.start()

    def outgoing(side, part, shift, slots):
        to = lax.rem(me + shift, devices)
        source, target = (to, me) if slots is None else (slots, slots)
        if part is None:
            source, target = send.at[side, source], recv.at[side, target]
        else:
            source, target = send.at[side, source, part], recv.at[side, target, part]
        number = part or 0
        return pltpu.make_async_remote_copy(
            src_ref=source, dst_ref=target,
            send_sem=send_sem.at[side, number], recv_sem=recv_sem.at[side, number],
            device_id={"row": to}, device_id_type=pl.DeviceIdType.MESH,
        )

    def returning(side, pair, shift, slots):
        to = lax.rem(me + shift, devices)
        source, target = (to, me) if slots is None else (slots, slots)
        if pair is None:
            source, target = back.at[side, source], home.at[side, target]
        else:
            source, target = back.at[side, source, pair], home.at[side, target, pair]
        number = pair or 0
        return pltpu.make_async_remote_copy(
            src_ref=source, dst_ref=target,
            send_sem=back_sem.at[side, number], recv_sem=home_sem.at[side, number],
            device_id={"row": to}, device_id_type=pl.DeviceIdType.MESH,
        )

    def turned_parts(one, two):
        last = jnp.concatenate([one[LANES:], two[LANES:]], axis=0)
        return [part.T for part in (one[:LANES], two[:LANES], last)]

    def keep(tile, one):
        left = lax.broadcasted_iota(jnp.int32, tile.shape, 1) < rest
        return jnp.where(left if one == 0 else jnp.logical_not(left), tile, 0.0)

    for load in loads[:5]:
        load.wait()
    for number in range(3):
        gains[number] = jnp.broadcast_to(gain_ref[number : number + 1, :], (feats, width)).T
    live = jnp.where(present_ref[...] > 0, 0.0, masked_score)
    bias_f[...] = jnp.broadcast_to(live, (feats, feats)).T
    prepare_weights(feat_qkv_ref, turned_f, spread_f)
    out_f[...] = turn(feat_out_ref[...], width)

    def gain_of(number):
        return jnp.concatenate([gains[number], gains[number]], axis=1)

    def feature_rows(step):
        cells = jnp.concatenate([mid[2 * step], mid[2 * step + 1]], axis=1)
        normed = norm_down(cells, gain_of(0)).astype(jnp.bfloat16)
        turned = matmul(turned_f[...], normed)
        keys = matmul(normed, spread_f[...], (0, 0))
        contexts = attention(turned, keys, bias_f)
        context = jnp.concatenate(contexts, axis=1).astype(jnp.bfloat16)
        updated = cells + matmul(out_f[...], context)
        mid[2 * step] = updated[:, :feats]
        mid[2 * step + 1] = updated[:, feats:]
        normed = norm_down(updated, gain_of(1))
        parts = turned_parts(normed[:, :feats], normed[:, feats:])
        part, inner = 2 * step // half, 2 * step % half
        for side in range(2):
            here = slice(side * group, (side + 1) * group)
            for one in range(2):
                sort_a[part, side, pl.ds(inner + one, group, stride=half), :] = parts[one][here]
            sort_b[part, side, pl.ds(inner // 2, group, stride=half // 2), :] = parts[2][here]

    def dispatch(side, part):
        for shift in order:
            outgoing(side, part, shift, None).start()

    for part in range(2):
        if part == 1:
            loads[5].wait()
        for step in range(part * steps // 2, (part + 1) * steps // 2):
            feature_rows(step)
        for side in range(2):
            first = sort_a[part, side].reshape(devices, share * half, LANES)
            last = sort_b[part, side].reshape(devices, share * half // 2, LANES)
            send[side, :, part, : share * half] = first.astype(jnp.bfloat16)
            send[side, :, part, share * half :] = last.astype(jnp.bfloat16)
        if part == 0:
            pl.semaphore_wait(barrier, devices - 1)
            dispatch(0, 0)
    dispatch(0, 1)
    dispatch(1, None)
    for side in range(2):
        recv[side, me] = send[side, me]

    for load in loads[6:]:
        load.wait()
    prepare_weights(item_qkv_ref, turned_i, spread_i)
    out_i[...] = turn(item_out_ref[...], out_i.shape[1])
    into[...] = turn(mlp_in_ref[...], width)
    left = lax.broadcasted_iota(jnp.int32, (1, feats), 1) < group
    for step in range(steps):
        one, two = mid[2 * step], mid[2 * step + 1]
        paired[0, step] = jnp.where(left, one, pltpu.roll(two, group, axis=1))
        paired[1, step] = jnp.where(left, pltpu.roll(one, group, axis=1), two)
    token = lax.broadcasted_iota(jnp.int32, (total_rows, total_rows), 0)
    number = token % devices * rows + token // devices
    bias_i[...] = jnp.where(number < n_train_ref[0], 0.0, masked_score)

    def item_side(side):
        for part in range(2):
            if side == 0:
                outgoing(0, part, 1, others).wait_recv()
            elif part == 0:
                outgoing(1, None, 1, others).wait_recv()
            tiles = recv[side, :, part].astype(jnp.float32)
            for device in range(devices):
                start = (device * 2 + part) * share * half
                loose_a[start : start + share * half, :] = tiles[device, : share * half]
                for one in range(2):
                    put = pl.ds(start + one, share * half // 2, stride=2)
                    loose_b[put, :] = keep(tiles[device, share * half :], one)

        def collect(feature):
            pieces = []
            for row in range(rows):
                start = (row // half) * share * half + feature * half + row % half
                take = pl.ds(start, devices, stride=2 * share * half)
                pieces.append(jnp.concatenate([loose_a[take, :], loose_b[take, :]], axis=1))
            return jnp.concatenate(pieces, axis=0)

        for pair in range(2):
            normed = jnp.concatenate([collect(2 * pair), collect(2 * pair + 1)], axis=0)
            normed = normed.astype(jnp.bfloat16)
            turned = matmul(turned_i[...], normed, (1, 1))
            keys = matmul(normed, spread_i[...])
            parts = turned_parts(*attention(turned, keys, bias_i))
            for number, part in enumerate(parts):
                sort_i[pair, number] = part
            for device in range(devices):
                take = pl.ds(device, rows, stride=devices)
                tile = jnp.concatenate([sort_i[pair, n, take, :] for n in range(3)], axis=0)
                back[side, device, pair] = tile.astype(jnp.bfloat16)
            if side == 0 or pair == 1:
                for shift in order:
                    returning(side, pair if side == 0 else None, shift, None).start()
        home[side, me] = back[side, me]

    for side in range(2):
        item_side(side)

    def finish_side(side):
        for pair in range(2):
            if side == 0:
                returning(0, pair, 1, others).wait_recv()
            elif pair == 0:
                returning(1, None, 1, others).wait_recv()
            tiles = home[side, :, pair].astype(jnp.float32)
            for device in range(devices):
                for one in range(2):
                    start = (device * share + 2 * pair + one) * rows
                    loose_a[start : start + rows, :] = tiles[device, one * rows : (one + 1) * rows]
                    loose_b[start : start + rows, :] = keep(tiles[device, 2 * rows :], one)
        for first in range(0, rows, 4):
            chosen = range(first, first + 4)
            context = []
            for row in chosen:
                take = pl.ds(row, group, stride=rows)
                context.append(jnp.concatenate([loose_a[take, :], loose_b[take, :]], axis=1))
            context = jnp.concatenate(context, axis=0).astype(jnp.bfloat16)
            stream = jnp.concatenate([paired[side, row // 2] for row in chosen[::2]], axis=1)
            late = stream + matmul(out_i[...], context, (1, 1))
            normed = norm_down(late, gain_of(2)).astype(jnp.bfloat16)
            inner = matmul(into[...], normed)
            hidden = (0.5 * inner * (1.0 + lax.erf(inner * math.sqrt(0.5)))).astype(jnp.bfloat16)
            done = late + matmul(mlp_out_ref[...], hidden)
            for number, row in enumerate(chosen[::2]):
                one = done[:, number * feats : (number + 1) * feats]
                two = pltpu.roll(one, group, axis=1)
                if side == 0:
                    out_ref[row] = one
                    out_ref[row + 1] = two
                else:
                    out_ref[row] = jnp.where(left, out_ref[row], two)
                    out_ref[row + 1] = jnp.where(left, out_ref[row + 1], one)

    for side in range(2):
        finish_side(side)
    for side, part in ((0, 0), (0, 1), (1, None)):
        outgoing(side, part, 1, others).wait_send()
    for side, pair in ((0, 0), (0, 1), (1, None)):
        returning(side, pair, 1, others).wait_send()


def body(
    cells, n_train, present, norm_gain, feat_qkv, feat_out, item_qkv, item_out, mlp_in, mlp_out
):
    devices = lax.axis_size("row")
    rows, feats, width = cells.shape
    feat_dev = feats // devices
    fits = rows == SUBLANES and feat_dev == SUBLANES and 2 * width == 3 * LANES and width == 32 * HEADS
    fits = fits and rows * devices == LANES and feats == LANES and width % (HEADS * 16) == 0
    if not fits:
        return plain_body(
            cells, n_train, present, norm_gain, feat_qkv, feat_out, item_qkv, item_out, mlp_in,
            mlp_out,
        )
    total_rows = rows * devices
    hidden = mlp_in.shape[1]
    total = 2 * LANES
    vmem = pl.BlockSpec(memory_space=pltpu.VMEM)
    hbm = pl.BlockSpec(memory_space=pltpu.HBM)
    bf16, f32 = jnp.bfloat16, jnp.float32
    slots = pltpu.VMEM((2, devices, 2, 3 * rows, LANES), bf16)
    sems = pltpu.SemaphoreType.DMA((2, 2))
    loose = pltpu.VMEM((rows * feats // 2, LANES), f32)
    arrays = (
        jnp.swapaxes(cells, 1, 2), present.reshape(1, feats), norm_gain, feat_qkv, feat_out,
        item_qkv, item_out, mlp_in, mlp_out.T,
    )
    arrays = [pltpu.with_memory_space_constraint(array, pltpu.HBM) for array in arrays]
    out = pl.pallas_call(
        functools.partial(kernel, devices),
        out_shape=jax.ShapeDtypeStruct((rows, width, feats), f32),
        in_specs=[pl.BlockSpec(memory_space=pltpu.SMEM)] + [hbm] * 9,
        out_specs=vmem,
        scratch_shapes=[
            pltpu.VMEM((1, feats), jnp.int32),
            pltpu.VMEM((3, width), f32),
            pltpu.VMEM((3, width, width), bf16),
            pltpu.VMEM((width, width), bf16),
            pltpu.VMEM((3, width, width), bf16),
            pltpu.VMEM((width, width), bf16),
            pltpu.VMEM((width, hidden), bf16),
            pltpu.VMEM((width, hidden), bf16),
            pltpu.VMEM((2 * width, width), bf16),
            pltpu.VMEM((width, 2 * width), bf16),
            pltpu.VMEM((2 * width, total), bf16),
            pltpu.VMEM((total, 2 * width), bf16),
            pltpu.VMEM((width, width), bf16),
            pltpu.VMEM((width, total), bf16),
            pltpu.VMEM((hidden, width), bf16),
            pltpu.VMEM((3, width, feats), f32),
            pltpu.VMEM((feats, feats), f32),
            pltpu.VMEM((total_rows, total_rows), f32),
            pltpu.VMEM((rows, width, feats), f32),
            pltpu.VMEM((2, rows // 2, width, feats), f32),
            pltpu.VMEM((2, 2, rows * feats // 4, LANES), f32),
            pltpu.VMEM((2, 2, rows * feats // 8, LANES), f32),
            pltpu.VMEM((2, 3, total_rows, LANES), f32),
            loose, loose, slots, slots, slots, slots,
            pltpu.SemaphoreType.DMA((10,)),
            sems, sems, sems, sems,
        ],
        compiler_params=pltpu.CompilerParams(
            collective_id=0, has_side_effects=True, vmem_limit_bytes=48 * 1024 * 1024
        ),
    )(n_train, *arrays)
    return jnp.swapaxes(out, 1, 2)


def solution(mesh):
    return jax.shard_map(
        body,
        mesh=mesh,
        in_specs=(
            P(("grp", "row"), None, None),
            P("grp"),
            P("grp"),
            P(),
            P(),
            P(),
            P(),
            P(),
            P(),
            P(),
        ),
        out_specs=P(("grp", "row"), None, None),
        check_vma=False,
    )
```

```python
import functools
import math

import jax
import jax.numpy as jnp
from jax import lax
from jax.experimental import pallas as pl
from jax.experimental.pallas import tpu as pltpu
from jax.sharding import PartitionSpec as P

HEADS = 6
LANES = 128
SUBLANES = 8


norm_floor = 0.25
masked_score = -1e30


def layer_norm(stream, gain):
    average = jnp.mean(stream, axis=-1, keepdims=True)
    centred = stream - average
    spread = jnp.mean(centred * centred, axis=-1, keepdims=True)
    return centred * lax.rsqrt(spread + norm_floor) * gain


def softmax_rows(scores):
    largest = jnp.max(scores, axis=-1, keepdims=True)
    exponent = jnp.exp(scores - largest)
    return exponent / jnp.sum(exponent, axis=-1, keepdims=True)


def plain_body(
    cells, n_train, present, norm_gain, feat_qkv, feat_out, item_qkv, item_out, mlp_in, mlp_out
):
    row_dev, feature_count, model_width = cells.shape
    devices_row = lax.axis_size("row")
    total_rows = row_dev * devices_row
    feat_dev = feature_count // devices_row
    head_size = model_width // HEADS
    scale = 1.0 / math.sqrt(head_size)
    query_rows = min(512, total_rows)
    highest = lax.Precision.HIGHEST
    normed = layer_norm(cells, norm_gain[0]).astype(jnp.bfloat16)
    triplet = jnp.einsum("rfe,ced->crfd", normed, feat_qkv, preferred_element_type=jnp.float32)
    triplet = triplet.reshape(3, row_dev, feature_count, HEADS, head_size)
    feat_values = triplet[2].astype(jnp.bfloat16)
    scores = jnp.einsum("rfhd,rghd->rhfg", triplet[0], triplet[1], precision=highest) * scale
    scores = jnp.where(present[None, None, None, :] > 0, scores, masked_score)
    weights = softmax_rows(scores).astype(jnp.bfloat16)
    context = jnp.einsum(
        "rhfg,rghd->rfhd", weights, feat_values, preferred_element_type=jnp.float32
    ).astype(jnp.bfloat16)
    context = context.reshape(row_dev, feature_count, model_width)
    cells_mid = cells + jnp.dot(context, feat_out, preferred_element_type=jnp.float32)
    key_live = lax.iota(jnp.int32, total_rows) < n_train[0]
    arrived = lax.all_to_all(
        cells_mid.reshape(row_dev, devices_row, feat_dev, model_width).astype(jnp.bfloat16),
        "row",
        split_axis=1,
        concat_axis=0,
        tiled=True,
    ).astype(jnp.float32)
    members = arrived.shape[2]
    stream = arrived.reshape(total_rows, members, model_width)
    normed_rows = layer_norm(stream, norm_gain[1]).astype(jnp.bfloat16)
    triples = jnp.einsum("rke,ced->kcrd", normed_rows, item_qkv, preferred_element_type=jnp.float32)

    def one_feature(triple):
        keys = triple[1].reshape(total_rows, HEADS, head_size)
        values = triple[2].astype(jnp.bfloat16).reshape(total_rows, HEADS, head_size)
        queries = triple[0].reshape(total_rows // query_rows, query_rows, HEADS, head_size)

        def query_group(chosen):
            group_scores = jnp.einsum("qhd,shd->hqs", chosen, keys, precision=highest) * scale
            group_scores = jnp.where(key_live[None, None, :], group_scores, masked_score)
            group_weights = softmax_rows(group_scores).astype(jnp.bfloat16)
            return jnp.einsum(
                "hqs,shd->qhd", group_weights, values, preferred_element_type=jnp.float32
            ).astype(jnp.bfloat16)

        return lax.map(query_group, queries).reshape(total_rows, model_width)

    gathered = lax.map(one_feature, triples)
    late = stream + jnp.dot(
        jnp.transpose(gathered, (1, 0, 2)), item_out, preferred_element_type=jnp.float32
    )
    normed_late = layer_norm(late, norm_gain[2]).astype(jnp.bfloat16)
    hidden = jax.nn.gelu(
        jnp.dot(normed_late, mlp_in, preferred_element_type=jnp.float32), approximate=False
    ).astype(jnp.bfloat16)
    updated = late + jnp.dot(hidden, mlp_out, preferred_element_type=jnp.float32)
    returned = lax.all_to_all(
        updated.reshape(total_rows, 1, members, model_width).astype(jnp.bfloat16),
        "row",
        split_axis=0,
        concat_axis=1,
        tiled=True,
    ).astype(jnp.float32)
    return returned.reshape(row_dev, feature_count, model_width)


def matmul(left, right, dims=(1, 0)):
    return lax.dot_general(
        left, right, (((dims[0],), (dims[1],)), ((), ())), preferred_element_type=jnp.float32
    )


def pick_rows(width, total):
    down = lax.broadcasted_iota(jnp.int32, (width, total), 0)
    across = lax.broadcasted_iota(jnp.int32, (width, total), 1)
    source = jnp.where(across < width, across, across - (total - width))
    return jnp.where(down == source, 1.0, 0.0).astype(jnp.bfloat16)


def turn(weight, total):
    return matmul(weight, pick_rows(weight.shape[0], total), (0, 0)).astype(jnp.bfloat16)


def prepare_weights(qkv_ref, turned_ref, spread_ref):
    width = qkv_ref.shape[1]
    total = turned_ref.shape[1]
    head = width // HEADS
    turned_ref[:width, :] = turn(qkv_ref[0], total)
    turned_ref[width:, :] = turn(qkv_ref[2], total)
    down = lax.broadcasted_iota(jnp.int32, (width, 2 * width), 0)
    across = lax.broadcasted_iota(jnp.int32, (width, 2 * width), 1)
    source = (across // (2 * head)) * head + across % head
    pick = jnp.where(down == source, 1.0, 0.0).astype(jnp.bfloat16)
    spread = matmul(qkv_ref[1], pick).astype(jnp.bfloat16)
    spread_ref[:width, :] = spread
    if total > width:
        spread_ref[width:, :] = spread[2 * width - total :]


def split(wide):
    high = wide.astype(jnp.bfloat16)
    return high, (wide - high.astype(jnp.float32)).astype(jnp.bfloat16)


def attention(turned, keys, bias_ref):
    width = turned.shape[0] // 2
    tokens = turned.shape[1]
    size = bias_ref.shape[0]
    head = width // HEADS
    query_high, query_low = split(turned[:width] * (math.log2(math.e) / math.sqrt(head)))
    key_high = keys.astype(jnp.bfloat16)
    bias = jnp.concatenate([bias_ref[...]] * (tokens // size), axis=0)
    lane = lax.broadcasted_iota(jnp.int32, keys.shape, 1)
    key_low = jnp.where(
        lane % (2 * head) < head,
        keys - key_high.astype(jnp.float32),
        jnp.concatenate([bias] * (HEADS // 2), axis=1),
    ).astype(jnp.bfloat16)
    down = lax.broadcasted_iota(jnp.int32, (head, size), 0)
    first = jnp.where(down == 0, 1.0, 0.0).astype(jnp.bfloat16)
    values = turned[width:].astype(jnp.bfloat16)
    zero = jnp.zeros((2 * head, size), jnp.bfloat16)
    blocks = []
    for block in range(tokens // size):
        here = slice(block * size, (block + 1) * size)
        contexts = []
        for pair in range(HEADS // 2):
            query = []
            for below in (query_low, None):
                for h in (2 * pair, 2 * pair + 1):
                    rows = slice(h * head, (h + 1) * head)
                    low = first if below is None else below[rows, here]
                    one = jnp.concatenate([query_high[rows, here], low], axis=0)
                    both = [one, zero] if h % 2 == 0 else [zero, one]
                    query.append(jnp.concatenate(both, axis=1))
            query = jnp.concatenate(query, axis=0)
            lanes = slice(pair * 4 * head, (pair + 1) * 4 * head)
            key = jnp.concatenate([key_high[here, lanes], key_low[here, lanes]], axis=1)
            both = matmul(key, query)
            for one in range(2):
                rows = slice((2 * pair + one) * head, (2 * pair + one + 1) * head)
                scores = both[:, one * size : (one + 1) * size]
                exponent = jnp.exp2(scores - jnp.max(scores, axis=0, keepdims=True))
                share = 1.0 / jnp.sum(exponent, axis=0, keepdims=True)
                weights = (exponent * share).astype(jnp.bfloat16)
                contexts.append(matmul(values[rows, here], weights))
        blocks.append(jnp.concatenate(contexts, axis=0))
    return blocks


def norm_down(stream, gain):
    average = jnp.mean(stream, axis=0, keepdims=True)
    centred = stream - average
    spread = jnp.mean(centred * centred, axis=0, keepdims=True)
    return centred * lax.rsqrt(spread + norm_floor) * gain


def kernel(
    devices,
    n_train_ref, cells_ref, present_hbm, gain_hbm, feat_qkv_hbm, feat_out_hbm, item_qkv_hbm,
    item_out_hbm, mlp_in_hbm, mlp_out_hbm,
    out_ref,
    present_ref, gain_ref, feat_qkv_ref, feat_out_ref, item_qkv_ref, item_out_ref, mlp_in_ref,
    mlp_out_ref, turned_f, spread_f, turned_i, spread_i, out_f, out_i, into, gains, bias_f, bias_i,
    mid, paired, sort_a, sort_b, sort_i, loose_a, loose_b, send, recv, back, home, in_sem, send_sem, recv_sem,
    back_sem, home_sem,
):
    me = lax.axis_index("row")
    rows, width, feats = cells_ref.shape
    steps = rows // 2
    half = rows // 2
    group = feats // 2
    share = group // devices
    total_rows = rows * devices
    rest = width - LANES
    order = range(1, devices)
    others = pl.ds(0, devices - 1)

    moves = [
        (gain_hbm, gain_ref), (present_hbm, present_ref), (feat_qkv_hbm, feat_qkv_ref),
        (cells_ref.at[pl.ds(0, half)], mid.at[pl.ds(0, half)]), (feat_out_hbm, feat_out_ref),
        (cells_ref.at[pl.ds(half, half)], mid.at[pl.ds(half, half)]),
        (item_qkv_hbm, item_qkv_ref), (item_out_hbm, item_out_ref), (mlp_in_hbm, mlp_in_ref),
        (mlp_out_hbm, mlp_out_ref),
    ]
    loads = [
        pltpu.make_async_copy(source, target, in_sem.at[number])
        for number, (source, target) in enumerate(moves)
    ]
    for load in loads[:5]:
        load.start()

    barrier = pltpu.get_barrier_semaphore()
    for shift in order:
        pl.semaphore_signal(
            barrier, inc=1, device_id={"row": lax.rem(me + shift, devices)},
            device_id_type=pl.DeviceIdType.MESH,
        )
    for load in loads[5:]:
        load.start()

    def outgoing(side, part, shift, slots):
        to = lax.rem(me + shift, devices)
        source, target = (to, me) if slots is None else (slots, slots)
        if part is None:
            source, target = send.at[side, source], recv.at[side, target]
        else:
            source, target = send.at[side, source, part], recv.at[side, target, part]
        number = part or 0
        return pltpu.make_async_remote_copy(
            src_ref=source, dst_ref=target,
            send_sem=send_sem.at[side, number], recv_sem=recv_sem.at[side, number],
            device_id={"row": to}, device_id_type=pl.DeviceIdType.MESH,
        )

    def returning(side, pair, shift, slots):
        to = lax.rem(me + shift, devices)
        source, target = (to, me) if slots is None else (slots, slots)
        if pair is None:
            source, target = back.at[side, source], home.at[side, target]
        else:
            source, target = back.at[side, source, pair], home.at[side, target, pair]
        number = pair or 0
        return pltpu.make_async_remote_copy(
            src_ref=source, dst_ref=target,
            send_sem=back_sem.at[side, number], recv_sem=home_sem.at[side, number],
            device_id={"row": to}, device_id_type=pl.DeviceIdType.MESH,
        )

    def turned_parts(one, two):
        last = jnp.concatenate([one[LANES:], two[LANES:]], axis=0)
        return [part.T for part in (one[:LANES], two[:LANES], last)]

    def keep(tile, one):
        left = lax.broadcasted_iota(jnp.int32, tile.shape, 1) < rest
        return jnp.where(left if one == 0 else jnp.logical_not(left), tile, 0.0)

    for load in loads[:5]:
        load.wait()
    for number in range(3):
        gains[number] = jnp.broadcast_to(gain_ref[number : number + 1, :], (feats, width)).T
    live = jnp.where(present_ref[...] > 0, 0.0, masked_score)
    bias_f[...] = jnp.broadcast_to(live, (feats, feats)).T
    prepare_weights(feat_qkv_ref, turned_f, spread_f)
    out_f[...] = turn(feat_out_ref[...], width)

    def gain_of(number):
        return jnp.concatenate([gains[number], gains[number]], axis=1)

    def feature_rows(step):
        cells = jnp.concatenate([mid[2 * step], mid[2 * step + 1]], axis=1)
        normed = norm_down(cells, gain_of(0)).astype(jnp.bfloat16)
        turned = matmul(turned_f[...], normed)
        keys = matmul(normed, spread_f[...], (0, 0))
        contexts = attention(turned, keys, bias_f)
        context = jnp.concatenate(contexts, axis=1).astype(jnp.bfloat16)
        updated = cells + matmul(out_f[...], context)
        mid[2 * step] = updated[:, :feats]
        mid[2 * step + 1] = updated[:, feats:]
        normed = norm_down(updated, gain_of(1))
        parts = turned_parts(normed[:, :feats], normed[:, feats:])
        part, inner = 2 * step // half, 2 * step % half
        for side in range(2):
            here = slice(side * group, (side + 1) * group)
            for one in range(2):
                sort_a[part, side, pl.ds(inner + one, group, stride=half), :] = parts[one][here]
            sort_b[part, side, pl.ds(inner // 2, group, stride=half // 2), :] = parts[2][here]

    def dispatch(side, part):
        for shift in order:
            outgoing(side, part, shift, None).start()

    for part in range(2):
        if part == 1:
            loads[5].wait()
        for step in range(part * steps // 2, (part + 1) * steps // 2):
            feature_rows(step)
        for side in range(2):
            first = sort_a[part, side].reshape(devices, share * half, LANES)
            last = sort_b[part, side].reshape(devices, share * half // 2, LANES)
            send[side, :, part, : share * half] = first.astype(jnp.bfloat16)
            send[side, :, part, share * half :] = last.astype(jnp.bfloat16)
        if part == 0:
            pl.semaphore_wait(barrier, devices - 1)
            dispatch(0, 0)
    dispatch(0, 1)
    dispatch(1, None)
    for side in range(2):
        recv[side, me] = send[side, me]

    for load in loads[6:]:
        load.wait()
    prepare_weights(item_qkv_ref, turned_i, spread_i)
    out_i[...] = turn(item_out_ref[...], out_i.shape[1])
    into[...] = turn(mlp_in_ref[...], width)
    left = lax.broadcasted_iota(jnp.int32, (1, feats), 1) < group
    for step in range(steps):
        one, two = mid[2 * step], mid[2 * step + 1]
        paired[0, step] = jnp.where(left, one, pltpu.roll(two, group, axis=1))
        paired[1, step] = jnp.where(left, pltpu.roll(one, group, axis=1), two)
    token = lax.broadcasted_iota(jnp.int32, (total_rows, total_rows), 0)
    number = token % devices * rows + token // devices
    bias_i[...] = jnp.where(number < n_train_ref[0], 0.0, masked_score)

    def item_side(side):
        for part in range(2):
            if side == 0:
                outgoing(0, part, 1, others).wait_recv()
            elif part == 0:
                outgoing(1, None, 1, others).wait_recv()
            tiles = recv[side, :, part].astype(jnp.float32)
            for device in range(devices):
                start = (device * 2 + part) * share * half
                loose_a[start : start + share * half, :] = tiles[device, : share * half]
                for one in range(2):
                    put = pl.ds(start + one, share * half // 2, stride=2)
                    loose_b[put, :] = keep(tiles[device, share * half :], one)

        def collect(feature):
            pieces = []
            for row in range(rows):
                start = (row // half) * share * half + feature * half + row % half
                take = pl.ds(start, devices, stride=2 * share * half)
                pieces.append(jnp.concatenate([loose_a[take, :], loose_b[take, :]], axis=1))
            return jnp.concatenate(pieces, axis=0)

        for pair in range(2):
            normed = jnp.concatenate([collect(2 * pair), collect(2 * pair + 1)], axis=0)
            normed = normed.astype(jnp.bfloat16)
            turned = matmul(turned_i[...], normed, (1, 1))
            keys = matmul(normed, spread_i[...])
            parts = turned_parts(*attention(turned, keys, bias_i))
            for number, part in enumerate(parts):
                sort_i[pair, number] = part
            for device in range(devices):
                take = pl.ds(device, rows, stride=devices)
                tile = jnp.concatenate([sort_i[pair, n, take, :] for n in range(3)], axis=0)
                back[side, device, pair] = tile.astype(jnp.bfloat16)
            if side == 0 or pair == 1:
                for shift in order:
                    returning(side, pair if side == 0 else None, shift, None).start()
        home[side, me] = back[side, me]

    for side in range(2):
        item_side(side)

    def finish_side(side):
        for pair in range(2):
            if side == 0:
                returning(0, pair, 1, others).wait_recv()
            elif pair == 0:
                returning(1, None, 1, others).wait_recv()
            tiles = home[side, :, pair].astype(jnp.float32)
            for device in range(devices):
                for one in range(2):
                    start = (device * share + 2 * pair + one) * rows
                    loose_a[start : start + rows, :] = tiles[device, one * rows : (one + 1) * rows]
                    loose_b[start : start + rows, :] = keep(tiles[device, 2 * rows :], one)
        for first in range(0, rows, 4):
            chosen = range(first, first + 4)
            context = []
            for row in chosen:
                take = pl.ds(row, group, stride=rows)
                context.append(jnp.concatenate([loose_a[take, :], loose_b[take, :]], axis=1))
            context = jnp.concatenate(context, axis=0).astype(jnp.bfloat16)
            stream = jnp.concatenate([paired[side, row // 2] for row in chosen[::2]], axis=1)
            late = stream + matmul(out_i[...], context, (1, 1))
            normed = norm_down(late, gain_of(2)).astype(jnp.bfloat16)
            inner = matmul(into[...], normed)
            hidden = (0.5 * inner * (1.0 + lax.erf(inner * math.sqrt(0.5)))).astype(jnp.bfloat16)
            done = late + matmul(mlp_out_ref[...], hidden)
            for number, row in enumerate(chosen[::2]):
                one = done[:, number * feats : (number + 1) * feats]
                two = pltpu.roll(one, group, axis=1)
                if side == 0:
                    out_ref[row] = one
                    out_ref[row + 1] = two
                else:
                    out_ref[row] = jnp.where(left, out_ref[row], two)
                    out_ref[row + 1] = jnp.where(left, out_ref[row + 1], one)

    for side in range(2):
        finish_side(side)
    for side, part in ((0, 0), (0, 1), (1, None)):
        outgoing(side, part, 1, others).wait_send()
    for side, pair in ((0, 0), (0, 1), (1, None)):
        returning(side, pair, 1, others).wait_send()


def body(
    cells, n_train, present, norm_gain, feat_qkv, feat_out, item_qkv, item_out, mlp_in, mlp_out
):
    devices = lax.axis_size("row")
    rows, feats, width = cells.shape
    feat_dev = feats // devices
    fits = rows == SUBLANES and feat_dev == SUBLANES and 2 * width == 3 * LANES and width == 32 * HEADS
    fits = fits and rows * devices == LANES and feats == LANES and width % (HEADS * 16) == 0
    if not fits:
        return plain_body(
            cells, n_train, present, norm_gain, feat_qkv, feat_out, item_qkv, item_out, mlp_in,
            mlp_out,
        )
    total_rows = rows * devices
    hidden = mlp_in.shape[1]
    total = 2 * LANES
    vmem = pl.BlockSpec(memory_space=pltpu.VMEM)
    hbm = pl.BlockSpec(memory_space=pltpu.HBM)
    bf16, f32 = jnp.bfloat16, jnp.float32
    slots = pltpu.VMEM((2, devices, 2, 3 * rows, LANES), bf16)
    sems = pltpu.SemaphoreType.DMA((2, 2))
    loose = pltpu.VMEM((rows * feats // 2, LANES), f32)
    arrays = (
        jnp.swapaxes(cells, 1, 2), present.reshape(1, feats), norm_gain, feat_qkv, feat_out,
        item_qkv, item_out, mlp_in, mlp_out.T,
    )
    arrays = [pltpu.with_memory_space_constraint(array, pltpu.HBM) for array in arrays]
    out = pl.pallas_call(
        functools.partial(kernel, devices),
        out_shape=jax.ShapeDtypeStruct((rows, width, feats), f32),
        in_specs=[pl.BlockSpec(memory_space=pltpu.SMEM)] + [hbm] * 9,
        out_specs=vmem,
        scratch_shapes=[
            pltpu.VMEM((1, feats), jnp.int32),
            pltpu.VMEM((3, width), f32),
            pltpu.VMEM((3, width, width), bf16),
            pltpu.VMEM((width, width), bf16),
            pltpu.VMEM((3, width, width), bf16),
            pltpu.VMEM((width, width), bf16),
            pltpu.VMEM((width, hidden), bf16),
            pltpu.VMEM((width, hidden), bf16),
            pltpu.VMEM((2 * width, width), bf16),
            pltpu.VMEM((width, 2 * width), bf16),
            pltpu.VMEM((2 * width, total), bf16),
            pltpu.VMEM((total, 2 * width), bf16),
            pltpu.VMEM((width, width), bf16),
            pltpu.VMEM((width, total), bf16),
            pltpu.VMEM((hidden, width), bf16),
            pltpu.VMEM((3, width, feats), f32),
            pltpu.VMEM((feats, feats), f32),
            pltpu.VMEM((total_rows, total_rows), f32),
            pltpu.VMEM((rows, width, feats), f32),
            pltpu.VMEM((2, rows // 2, width, feats), f32),
            pltpu.VMEM((2, 2, rows * feats // 4, LANES), f32),
            pltpu.VMEM((2, 2, rows * feats // 8, LANES), f32),
            pltpu.VMEM((2, 3, total_rows, LANES), f32),
            loose, loose, slots, slots, slots, slots,
            pltpu.SemaphoreType.DMA((10,)),
            sems, sems, sems, sems,
        ],
        compiler_params=pltpu.CompilerParams(
            collective_id=0, has_side_effects=True, vmem_limit_bytes=48 * 1024 * 1024
        ),
    )(n_train, *arrays)
    return jnp.swapaxes(out, 1, 2)


def solution(mesh):
    return jax.shard_map(
        body,
        mesh=mesh,
        in_specs=(
            P(("grp", "row"), None, None),
            P("grp"),
            P("grp"),
            P(),
            P(),
            P(),
            P(),
            P(),
            P(),
            P(),
        ),
        out_specs=P(("grp", "row"), None, None),
        check_vma=False,
    )
```
